32 devices in a mesh: dp: 4 (over y, core), tensor: 8 (over z, x).
Axes of the slice: x: 2, y: 2, z: 4, core: 2. Of those that a mesh axis runs over, the one named last changes fastest.
Arguments:
- grads: bfloat16 [4, 2, 7168, 2048], P('dp', None, 'tensor'), may hold values from -6 to 6
- master: float32 [2, 7168, 2048], P(None, 'dp', 'tensor'), may hold values from -0.0625 to 0.0625
- moment1: float32 [2, 7168, 2048], P(None, 'dp', 'tensor'), may hold values from -3 to 3
- moment2: float32 [2, 7168, 2048], P(None, 'dp', 'tensor'), may hold values from 1 to 30
- tokens: bfloat16 [1024, 7168], P('dp'), may hold values from -6 to 6
- route: int32 [512], P('dp'), may hold values from 0 to 255, as said below
Outputs:
- new_master: float32 [2, 7168, 2048], P(None, 'dp', 'tensor')
- new_moment1: float32 [2, 7168, 2048], P(None, 'dp', 'tensor')
- new_moment2: float32 [2, 7168, 2048], P(None, 'dp', 'tensor')
- rollout: bfloat16 [2, 7168, 2048], P(None, None, 'tensor')
- hidden: bfloat16 [512, 2048], P('dp', 'tensor')
The draws below stay inside these ranges and needn't reach their ends.
Inputs may be any that keep to these rules, and one draw needn't show every extreme that they name: route[i] indexes one of the 256 tokens of the data rank that holds routed row i; within one data rank's 128 routed rows no token appears twice.
All inputs are finite; a program needn't handle non-finite values.
Results may differ from the reference program's by a relative error of at most 0.019.
Values may be sent and summed in bfloat16 or wider, within the bound.
No kernel may reach another device: no remote copies, remote signals or barrier semaphores. Data moves between devices by JAX's collectives and lax.ppermute only.
A program may use at most 128 MiB of HBM per device.

```python
import math
import jax
import jax.numpy as jnp
from jax import lax

D = 7168
H = 2048
TOK_DEV = 256
ROUTED_DEV = 128
TOKENS = 1024
ROUTED = 512
N_DP = 4


def draw_route(key, part):
    rank_keys = jax.random.split(key, ROUTED // ROUTED_DEV)

    def one_rank(rank_key):
        order = jax.random.permutation(rank_key, TOK_DEV)
        return order[:ROUTED_DEV]
    chosen = jax.vmap(one_rank)(rank_keys)
    return chosen.reshape(ROUTED).astype(jnp.int32)


def spiked(entries, key, source, target, parts, factor):
    owner, partner = [(jnp.arange(entries.shape[axis_at]) // (entries.shape[axis_at] // parts)).reshape([-1 if axis == axis_at else 1 for axis in range(entries.ndim)]) for axis_at in (source, target)]
    chosen = jax.random.permutation(key, parts)[partner]
    strong = (owner == chosen) | (owner == (partner + parts // 2) % parts)
    return jnp.where(strong, factor * entries, entries)


def shard_levels(stream_key, shape, cuts, least, largest):
    loudness = 1.0
    for axis_at, shards_of in cuts:
        draws = jax.random.uniform(jax.random.fold_in(jax.random.fold_in(stream_key, 6), axis_at), (shards_of,), jnp.float32, least / len(cuts), largest / len(cuts))
        loudness = loudness * jnp.repeat(jnp.exp(draws), shape[axis_at] // shards_of).reshape((-1,) + (1,) * (len(shape) - 1 - axis_at))
    return loudness


def centred(rng, dims, width, reach, shards=(), held_as=jnp.bfloat16):
    array = jax.random.normal(rng, dims, jnp.float32) * width
    if len(shards) > 0:
        array = shard_levels(rng, dims, shards, -0.22, 0.18) * array
    return jnp.clip(array, min=-reach, max=reach).astype(held_as)


def noise_with(stream_key, extent, deviation, limit, cuts, heavy, kind=jnp.bfloat16):
    values = deviation * jax.random.normal(stream_key, extent, jnp.float32)
    if cuts:
        values = values * shard_levels(stream_key, extent, cuts, -0.22, 0.18)
    return jnp.clip(spiked(values, jax.random.fold_in(stream_key, 3), *heavy), -limit, limit).astype(kind)


def setup_inputs(seed: int = 0) -> dict:
    key_list = jax.random.split(jax.random.key(seed), 7)
    grads = noise_with(key_list[0], (N_DP, 2, D, H), 1.0, 6.0, ((0, 4), (2, 8)), (0, 2, 4, 2.0))
    master = centred(key_list[1], (2, D, H), D ** -0.5, 0.0625, ((1, 4), (2, 8)), jnp.float32)
    moment1 = centred(key_list[2], (2, D, H), 0.5, 3.0, ((1, 4), (2, 8)), jnp.float32)
    moment2 = jnp.clip(jnp.exp(math.log(30.0) - 3.4011974 * jax.random.uniform(key_list[3], (2, D, H), jnp.float32) ** shard_levels(key_list[3], (2, D, H), ((1, 4), (2, 8)), -0.2, 0.2)), 1.0, 30.0)
    tokens = centred(key_list[4], (TOKENS, D), 1.0, 6.0, ((0, 4),))
    route = draw_route(jax.random.fold_in(key_list[6], 71), 0)
    return {"grads": grads, "master": master, "moment1": moment1, "moment2": moment2, "tokens": tokens, "route": route}


def reference(grads, master, moment1, moment2, tokens, route):

    def accumulate(carry, piece):
        return (carry + piece.astype(jnp.float32), None)
    start = jnp.zeros(master.shape, jnp.float32)
    grad_total, _ = lax.scan(accumulate, start, grads)
    new_moment1 = 0.9 * moment1 + 0.1 * grad_total
    new_moment2 = 0.95 * moment2 + 0.05 * grad_total * grad_total
    first_fix = 1.0 - 0.9 ** 10
    second_fix = 1.0 - 0.95 ** 10
    step_size = new_moment1 / first_fix / (jnp.sqrt(new_moment2 / second_fix) + 1e-08) + 0.1 * master
    new_master = master - 0.003 * step_size
    rollout = new_master.astype(jnp.bfloat16)
    block = jnp.arange(ROUTED, dtype=jnp.int32) // ROUTED_DEV
    row_index = (block * TOK_DEV + route).astype(jnp.int32)
    picked = jnp.take(tokens, row_index, axis=0)
    gate_out = jnp.dot(picked, rollout[0], preferred_element_type=jnp.float32)
    up_out = jnp.dot(picked, rollout[1], preferred_element_type=jnp.float32)
    hidden = (jax.nn.silu(gate_out) * up_out).astype(jnp.bfloat16)
    return (new_master, new_moment1, new_moment2, rollout, hidden)
```

```python
import jax
import jax.numpy as jnp
from jax import lax
from jax.sharding import PartitionSpec as P


def bit_reverse(value, bits):
    out = value * 0
    for b in range(bits):
        out = out + ((value >> b) & 1) * (1 << (bits - 1 - b))
    return out


def flip(x, rank_count, b):
    return lax.ppermute(x, "dp", [(i, i ^ (1 << b)) for i in range(rank_count)])


def reduce_rows(part, rank, rank_count, bits):
    for b in range(bits):
        rows, width = part.shape
        halves = part.reshape(2, rows // 2, width)
        mine = (rank >> b) & 1
        send = lax.dynamic_index_in_dim(halves, 1 - mine, 0, keepdims=False)
        keep = lax.dynamic_index_in_dim(halves, mine, 0, keepdims=False)
        got = flip(send, rank_count, b)
        part = (keep.astype(jnp.float32) + got.astype(jnp.float32)).astype(jnp.bfloat16)
    return part


def exchange(part, rank_count, tensor_count, bits, col_index):
    slab, width = part.shape
    col = width // tensor_count
    m = tensor_count // rank_count
    rank = lax.axis_index("dp")
    base = m * bit_reverse(rank, bits) + col_index % m
    owned = jnp.zeros((m, rank_count, slab, col), part.dtype)
    for d in range(tensor_count):
        perm = []
        for r in range(rank_count):
            for s in range(tensor_count):
                t = (m * bit_reverse(r, bits) + s % m + d) % tensor_count
                perm.append((r * tensor_count + s, (s // m) * tensor_count + t))
        target = (base + d) % tensor_count
        piece = lax.dynamic_slice(part, (0, target * col), (slab, col))
        got = lax.ppermute(piece, ("dp", "tensor"), perm)
        v = (col_index - d) % tensor_count
        owned = lax.dynamic_update_slice(owned, got[None, None], (v % m, v // m, 0, 0))
    return owned.reshape(m * rank_count * slab, col)


def adam(total, master, moment1, moment2):
    total = total.astype(jnp.float32)
    new_moment1 = 0.9 * moment1 + 0.1 * total
    new_moment2 = 0.95 * moment2 + 0.05 * total * total
    first_fix = 1.0 - 0.9**10
    second_fix = 1.0 - 0.95**10
    step_size = (
        new_moment1 / first_fix / (jnp.sqrt(new_moment2 / second_fix) + 1e-08) + 0.1 * master
    )
    return master - 0.003 * step_size, new_moment1, new_moment2


def body(grads, master, moment1, moment2, tokens, route):
    tensor_count = lax.axis_size("tensor")
    rank_count = lax.axis_size("dp")
    bits = rank_count.bit_length() - 1
    rank = lax.axis_index("dp")
    col_index = lax.axis_index("tensor")
    stacked = master.shape[0]
    rows = master.shape[1]
    col = master.shape[2]

    picked = jnp.take(tokens, route, axis=0, mode="clip")
    totals, parts = [], []
    rollout = jnp.zeros((stacked, rank_count, rows, col), jnp.bfloat16)
    for k in range(stacked):
        part = reduce_rows(grads[0, k], rank, rank_count, bits)
        total = exchange(part, rank_count, tensor_count, bits, col_index)
        totals.append(total)
        own = adam(total, master[k], moment1[k], moment2[k])[0].astype(jnp.bfloat16)
        blocks = [(0, own)]
        for b in reversed(range(bits)):
            blocks = blocks + [(j ^ (1 << b), flip(x, rank_count, b)) for j, x in blocks]
        acc = 0.0
        for j, x in blocks:
            source = rank ^ j
            rollout = lax.dynamic_update_slice(rollout, x[None, None], (k, source, 0, 0))
            left = lax.dynamic_slice(picked, (0, source * rows), (picked.shape[0], rows))
            acc = acc + jnp.dot(left, x, preferred_element_type=jnp.float32)
        parts.append(acc)
    new_master, new_moment1, new_moment2 = adam(jnp.stack(totals), master, moment1, moment2)
    hidden = (jax.nn.silu(parts[0]) * parts[1]).astype(jnp.bfloat16)
    rollout = rollout.reshape(stacked, rank_count * rows, col)
    return (new_master, new_moment1, new_moment2, rollout, hidden)


def solution(mesh):
    in_specs = (
        P("dp", None, "tensor", None),
        P(None, "dp", "tensor"),
        P(None, "dp", "tensor"),
        P(None, "dp", "tensor"),
        P("dp", None),
        P("dp"),
    )
    out_specs = (
        P(None, "dp", "tensor"),
        P(None, "dp", "tensor"),
        P(None, "dp", "tensor"),
        P(None, None, "tensor"),
        P("dp", "tensor"),
    )
    return jax.shard_map(body, mesh=mesh, in_specs=in_specs, out_specs=out_specs, check_vma=False)
```

```python
import jax
import jax.numpy as jnp
from jax import lax
from jax.sharding import PartitionSpec as P


def bit_reverse(value, bits):
    out = value * 0
    for b in range(bits):
        out = out + ((value >> b) & 1) * (1 << (bits - 1 - b))
    return out


def flip(x, rank_count, b):
    return lax.ppermute(x, "dp", [(i, i ^ (1 << b)) for i in range(rank_count)])


def reduce_rows(grads, k, rank, rank_count, bits):
    stacked, rows, width = grads.shape
    halves = grads.reshape(stacked, 2, rows // 2, width)
    for b in range(bits):
        first = k if b == 0 else 0
        rows = rows // 2
        mine = (rank >> b) & 1
        size = (1, 1, rows, width)
        send = lax.dynamic_slice(halves, (first, 1 - mine, 0, 0), size)[0, 0]
        keep = lax.dynamic_slice(halves, (first, mine, 0, 0), size)[0, 0]
        got = flip(send, rank_count, b)
        part = (keep.astype(jnp.float32) + got.astype(jnp.float32)).astype(jnp.bfloat16)
        halves = part.reshape(1, 2, rows // 2, width) if b + 1 < bits else part
    return halves


def exchange(part, rank_count, tensor_count, bits, col_index):
    slab, width = part.shape
    col = width // tensor_count
    m = tensor_count // rank_count
    rank = lax.axis_index("dp")
    base = m * bit_reverse(rank, bits) + col_index % m
    owned = jnp.zeros((m, rank_count, slab, col), part.dtype)
    for d in range(tensor_count):
        perm = []
        for r in range(rank_count):
            for s in range(tensor_count):
                t = (m * bit_reverse(r, bits) + s % m + d) % tensor_count
                perm.append((r * tensor_count + s, (s // m) * tensor_count + t))
        target = (base + d) % tensor_count
        piece = lax.dynamic_slice(part, (0, target * col), (slab, col))
        got = lax.ppermute(piece, ("dp", "tensor"), perm)
        v = (col_index - d) % tensor_count
        owned = lax.dynamic_update_slice(owned, got[None, None], (v % m, v // m, 0, 0))
    return owned.reshape(m * rank_count * slab, col)


def adam(total, master, moment1, moment2):
    total = total.astype(jnp.float32)
    new_moment1 = 0.9 * moment1 + 0.1 * total
    new_moment2 = 0.95 * moment2 + 0.05 * total * total
    first_fix = 1.0 - 0.9**10
    second_fix = 1.0 - 0.95**10
    step_size = (
        new_moment1 / first_fix / (jnp.sqrt(new_moment2 / second_fix) + 1e-08) + 0.1 * master
    )
    return master - 0.003 * step_size, new_moment1, new_moment2


def body(grads, master, moment1, moment2, tokens, route):
    tensor_count = lax.axis_size("tensor")
    rank_count = lax.axis_size("dp")
    bits = rank_count.bit_length() - 1
    rank = lax.axis_index("dp")
    col_index = lax.axis_index("tensor")
    stacked = master.shape[0]
    rows = master.shape[1]
    col = master.shape[2]

    picked = jnp.take(tokens, route, axis=0, mode="clip")
    slabs = [reduce_rows(grads[0], k, rank, rank_count, bits) for k in range(stacked)]
    zero, slabs[0] = lax.optimization_barrier((jnp.zeros((), jnp.bfloat16), slabs[0]))
    totals, parts, chains = [], [], []
    rollout = jnp.broadcast_to(zero, (stacked, rank_count, rows, col))
    own = None
    for k in range(stacked):
        slab = slabs[k]
        if own is not None:
            slab, own = lax.optimization_barrier((slab, own))
            chains.append(own)
        total = exchange(slab, rank_count, tensor_count, bits, col_index)
        totals.append(total)
        own = adam(total, master[k], moment1[k], moment2[k])[0].astype(jnp.bfloat16)
    chains.append(own)
    for k in range(stacked):
        blocks = [(0, chains[k])]
        for b in reversed(range(bits)):
            blocks = blocks + [(j ^ (1 << b), flip(x, rank_count, b)) for j, x in blocks]
        acc = 0.0
        for j, x in blocks:
            source = rank ^ j
            rollout = lax.dynamic_update_slice(rollout, x[None, None], (k, source, 0, 0))
            left = lax.dynamic_slice(picked, (0, source * rows), (picked.shape[0], rows))
            acc = acc + jnp.dot(left, x, preferred_element_type=jnp.float32)
        parts.append(acc)
    new_master, new_moment1, new_moment2 = adam(jnp.stack(totals), master, moment1, moment2)
    hidden = (jax.nn.silu(parts[0]) * parts[1]).astype(jnp.bfloat16)
    rollout = rollout.reshape(stacked, rank_count * rows, col)
    return (new_master, new_moment1, new_moment2, rollout, hidden)


def solution(mesh):
    in_specs = (
        P("dp", None, "tensor", None),
        P(None, "dp", "tensor"),
        P(None, "dp", "tensor"),
        P(None, "dp", "tensor"),
        P("dp", None),
        P("dp"),
    )
    out_specs = (
        P(None, "dp", "tensor"),
        P(None, "dp", "tensor"),
        P(None, "dp", "tensor"),
        P(None, None, "tensor"),
        P("dp", "tensor"),
    )
    return jax.shard_map(body, mesh=mesh, in_specs=in_specs, out_specs=out_specs, check_vma=False)
```
